32 devices in a mesh: row: 4 (over z), col: 8 (over y, x, core).
Axes of the slice: x: 2, y: 2, z: 4, core: 2. Of those that a mesh axis runs over, the one named last changes fastest.
Arguments:
- a_blocks: bfloat16 [8, 8, 43, 128, 128], P('col', 'row'), may hold values from -6 to 6
- a_index: int32 [8, 8, 43], P('col', 'row'), may hold values from 0 to 479, as said below
- b_blocks: bfloat16 [8, 8, 43, 128, 128], P('col', 'row'), may hold values from -0.5 to 0.5
- b_index: int32 [8, 8, 43], P('col', 'row'), may hold values from 0 to 479, as said below
- pair_list: int32 [8, 8, 3, 2, 40], P('col', 'row'), may hold values from 0 to 42, as said below
- pair_count: int32 [8, 8, 3], P('col', 'row'), may hold values from 0 to 40, as said below
Outputs:
- c_window: bfloat16 [10240, 10240], P('col', 'row')
The draws below stay inside these ranges and needn't reach their ends.
Inputs may be any that keep to these rules, and one draw needn't show every extreme that they name: a_index[p, k, j] = 10 * (block column) + (block row) of stored slot j in A panel (p, k); the slots of one panel hold distinct positions. b_index[k, q, j] = 10 * (block row) + (block column) of stored slot j in B panel (k, q); the slots of one panel hold distinct positions. `pair_list`: entry j < pair_count[p, q, s] of list (p, q, s) names a slot a of A panel (p, k) and a slot b of B panel (k, q), k = (p + q + s) mod 8, with a_index // 10 equal to b_index // 10; no pair twice in a list; entries from pair_count on are zero. `pair_count`: in every draw some list is full.
All inputs are finite; a program needn't handle non-finite values.
Results may differ from the reference program's by a relative error of at most 0.001.
Values may be sent and summed in bfloat16 or wider, within the bound.
A program may use at most 128 MiB of HBM per device.

```python
import jax
import jax.numpy as jnp
from jax import lax

BS = 128
KB = 48
WB = 10
STEPS = 3
PANELS = 8
CAP = 43
PAIRS = 40


def panel_ids(key, forced):
    slots = WB * KB
    spread = jax.random.permutation(key, slots).astype(jnp.int32)
    rest = jax.random.permutation(jax.random.fold_in(key, 3), slots - WB).astype(jnp.int32)
    leading = jnp.concatenate([jnp.arange(WB, dtype=jnp.int32), WB + rest])
    return jnp.where(forced, leading, spread)[:CAP]


def occupancy(key):
    base = jax.random.fold_in(key, 11)
    keys = jax.random.split(base, 8)
    row_pick = jax.random.randint(keys[0], (), 0, PANELS)
    col_pick = jax.random.randint(keys[1], (), 0, PANELS)
    inner_pick = (row_pick + col_pick) % PANELS
    first_axis = jnp.arange(PANELS)[:, None]
    second_axis = jnp.arange(PANELS)[None, :]
    forced_a = ((first_axis == row_pick) & (second_axis == inner_pick)).reshape(-1)
    forced_b = ((first_axis == inner_pick) & (second_axis == col_pick)).reshape(-1)
    a_ids = jax.vmap(panel_ids)(jax.random.split(keys[2], PANELS * PANELS), forced_a).reshape(PANELS, PANELS, CAP)
    b_ids = jax.vmap(panel_ids)(jax.random.split(keys[3], PANELS * PANELS), forced_b).reshape(PANELS, PANELS, CAP)
    flat_panels = jnp.arange(PANELS * PANELS).reshape(PANELS, PANELS)
    a_live = jax.random.randint(keys[4], (PANELS, PANELS), CAP // 2, CAP + 1)
    a_full = jax.random.randint(keys[5], (), 0, PANELS * PANELS)
    a_live = jnp.where(flat_panels == a_full, CAP, a_live)
    b_live = jax.random.randint(keys[6], (PANELS, PANELS), CAP // 2, CAP + 1)
    b_full = jax.random.randint(keys[7], (), 0, PANELS * PANELS)
    b_live = jnp.where(flat_panels == b_full, CAP, b_live)
    return (a_ids, a_live, b_ids, b_live)


def pair_tables(key):
    a_ids, a_live, b_ids, b_live = occupancy(key)

    def one_list(row_panel, col_panel, step_no):
        inner = (row_panel + col_panel + step_no) % PANELS
        slot_range = jnp.arange(CAP)
        a_inner = a_ids[row_panel, inner] // WB
        b_inner = b_ids[inner, col_panel] // WB
        matched = (slot_range[:, None] < a_live[row_panel, inner]) & (slot_range[None, :] < b_live[inner, col_panel]) & (a_inner[:, None] == b_inner[None, :])
        flat_pos = jnp.arange(CAP * CAP)
        ranked = jnp.sort(jnp.where(matched.reshape(-1), flat_pos, CAP * CAP + flat_pos))[:PAIRS]
        live_count = jnp.minimum(jnp.sum(matched.astype(jnp.int32)), PAIRS)
        is_live = jnp.arange(PAIRS) < live_count
        a_slots = jnp.where(is_live, ranked // CAP, 0)
        b_slots = jnp.where(is_live, ranked % CAP, 0)
        return (jnp.stack([a_slots, b_slots]).astype(jnp.int32), live_count.astype(jnp.int32))
    rows_grid, cols_grid, steps_grid = jnp.meshgrid(jnp.arange(PANELS), jnp.arange(PANELS), jnp.arange(STEPS), indexing='ij')
    lists, counts = jax.vmap(one_list)(rows_grid.reshape(-1), cols_grid.reshape(-1), steps_grid.reshape(-1))
    return (lists.reshape(PANELS, PANELS, STEPS, 2, PAIRS), counts.reshape(PANELS, PANELS, STEPS))


def draw_a_index(key, part):
    return occupancy(key)[0].astype(jnp.int32)


def draw_b_index(key, part):
    return occupancy(key)[2].astype(jnp.int32)


def draw_pair_list(key, part):
    return pair_tables(key)[0]


def draw_pair_count(key, part):
    return pair_tables(key)[1]


def steps_of(key, extent, pieces, smallest, top_value):
    def one(axis_at, parts):
        steps = jax.random.uniform(jax.random.fold_in(jax.random.fold_in(key, 6), axis_at), (parts,), jnp.float32, smallest / len(pieces), top_value / len(pieces))
        return jnp.repeat(jnp.exp(steps), extent[axis_at] // parts).reshape((-1,) + (1,) * (len(extent) - axis_at - 1))

    level = one(*pieces[0])
    for cut in pieces[1:]:
        level = level * one(*cut)
    return level


def normal_values(own_key, shape, scale, limit, pieces=(), kind=jnp.bfloat16):
    entries = jax.random.normal(own_key, shape, jnp.float32) * scale
    if len(pieces) > 0:
        entries = steps_of(own_key, shape, pieces, -0.22, 0.18) * entries
    return jnp.clip(entries, min=-limit, max=limit).astype(kind)


def setup_inputs(seed: int = 0) -> dict:
    arg_keys = jax.random.split(jax.random.key(seed), 7)
    a_blocks = normal_values(arg_keys[0], (PANELS, PANELS, CAP, BS, BS), 1.0, 6.0, ((0, 8), (1, 4)))
    a_index = draw_a_index(jax.random.fold_in(arg_keys[6], 71), 0)
    b_blocks = normal_values(arg_keys[2], (PANELS, PANELS, CAP, BS, BS), BS ** -0.5, 0.5, ((0, 8), (1, 4)))
    b_index = draw_b_index(jax.random.fold_in(arg_keys[6], 71), 0)
    pair_list = draw_pair_list(jax.random.fold_in(arg_keys[6], 71), 0)
    pair_count = draw_pair_count(jax.random.fold_in(arg_keys[6], 71), 0)
    return dict(a_blocks=a_blocks, a_index=a_index, b_blocks=b_blocks, b_index=b_index, pair_list=pair_list, pair_count=pair_count)


def panel_product(a_blocks, a_index, b_blocks, b_index, pair_list, pair_count, row_panel, col_panel):
    panels = a_blocks.shape[0]
    edge = a_blocks.shape[-1]
    running = jnp.zeros((WB * WB, edge, edge), jnp.float32)
    for step_no in range(STEPS):
        inner = ((row_panel + col_panel + step_no) % panels).astype(jnp.int32)
        a_slots = pair_list[row_panel, col_panel, step_no, 0].astype(jnp.int32)
        b_slots = pair_list[row_panel, col_panel, step_no, 1].astype(jnp.int32)
        is_live = (jnp.arange(a_slots.shape[0], dtype=jnp.int32) < pair_count[row_panel, col_panel, step_no]).astype(jnp.float32)
        lhs_blocks = a_blocks[row_panel, inner][a_slots].astype(jnp.float32)
        rhs_blocks = b_blocks[inner, col_panel][b_slots].astype(jnp.float32)
        products = jnp.einsum("pij,pjk->pik", lhs_blocks, rhs_blocks) * is_live[:, None, None]
        target = (a_index[row_panel, inner][a_slots] % WB) * WB + b_index[inner, col_panel][b_slots] % WB
        running = running + jax.ops.segment_sum(products, target.astype(jnp.int32), num_segments=WB * WB)
    grid = running.reshape(WB, WB, edge, edge).transpose(0, 2, 1, 3).reshape(WB * edge, WB * edge)
    return grid.astype(jnp.bfloat16)


def reference(a_blocks, a_index, b_blocks, b_index, pair_list, pair_count):
    panels = a_blocks.shape[0]
    columns = a_blocks.shape[1]
    edge = a_blocks.shape[-1]

    def one_row(row_panel):
        def one_col(col_panel):
            return panel_product(a_blocks, a_index, b_blocks, b_index, pair_list, pair_count, row_panel, col_panel)
        return lax.map(one_col, jnp.arange(columns, dtype=jnp.int32))

    stacked = lax.map(one_row, jnp.arange(panels, dtype=jnp.int32))
    return stacked.transpose(0, 2, 1, 3).reshape(panels * WB * edge, columns * WB * edge)
```

```python
import functools

import jax
import jax.numpy as jnp
from jax import lax
from jax.experimental import pallas as pl
from jax.experimental.pallas import tpu as pltpu
from jax.sharding import PartitionSpec as P

WB = 10
MESH = pl.DeviceIdType.MESH
ANY = pl.BlockSpec(memory_space=pl.ANY)
SMEM = pl.BlockSpec(memory_space=pltpu.SMEM)


def move_kernel(rows, cols, steps, a_ref, ai_ref, b_ref, bi_ref, ao_ref, aio_ref, bo_ref, bio_ref,
                a_recv, a_down, a_up, ai_recv, ai_send, b_recv, b_send, b_pass, bi_recv, bi_send, own):
    p = lax.axis_index("col")
    r = lax.axis_index("row")
    panels = 2 * rows
    span = steps + 1
    sends = []

    def remote(src, dst, send_sem, recv_sem, device):
        return pltpu.make_async_remote_copy(
            src_ref=src, dst_ref=dst, send_sem=send_sem, recv_sem=recv_sem,
            device_id=device, device_id_type=MESH)

    def go(cond, copy):
        @pl.when(cond)
        def _():
            copy.start()
        sends.append((cond, copy))

    def needed(k, row):
        return lax.rem(k - p - 2 * row + 2 * panels + cols, panels) < span

    def carried(k, lo, hi):
        total = 0
        for row in range(rows):
            hit = needed(k, row) & (row >= lo) & (row <= hi)
            total = total + jnp.where(hit, 1, 0)
        return total > 0

    own_a = pltpu.make_async_copy(ai_ref, aio_ref.at[r], own.at[0])
    own_a.start()
    for d in range(1, rows):
        to = lax.rem(r + d, rows)
        go(r >= 0, remote(ai_ref, aio_ref.at[r], ai_send.at[d], ai_recv.at[d], {"row": to}))
    own_slot = lax.rem(2 * cols - 2 * r, cols)
    for j in range(span):
        to = lax.rem(p - 2 * r - j + 2 * cols, cols)
        go(to != p, remote(bi_ref, bio_ref.at[j], bi_send.at[j], bi_recv.at[j], {"col": to}))

        @pl.when(own_slot == j)
        def _():
            keep = pltpu.make_async_copy(bi_ref, bio_ref.at[j], own.at[1])
            keep.start()
            keep.wait()

    def a_pair(k, h, d, src):
        def down(cond):
            go(cond & (r >= 1) & carried(k, 0, r - 1),
               remote(src, ao_ref.at[k], a_down.at[d, h], a_recv.at[k], {"row": lax.max(r - 1, 0)}))

        def up(cond):
            go(cond & (r <= rows - 2) & carried(k, r + 1, rows - 1),
               remote(src, ao_ref.at[k], a_up.at[d, h], a_recv.at[k], {"row": lax.min(r + 1, rows - 1)}))
        return down, up

    for h in range(2):
        k = 2 * r + h
        down, up = a_pair(k, h, 0, a_ref.at[h])
        down(r >= 0)
        up(r >= 0)
    for h in range(2):
        base = lax.rem(p - 2 * r - h + 2 * cols, cols)
        near = lax.rem(base - 1 + cols, cols)
        odd = lax.rem(base, 2)
        far = lax.rem(base - 2 * odd + cols, cols)
        go(near != p, remote(b_ref.at[h], bo_ref.at[h, 1], b_send.at[h, 0], b_recv.at[h, 1], {"col": near}))
        go(far != p, remote(b_ref.at[h], bo_ref.at[h, 2 * odd], b_send.at[h, 1], b_recv.at[h, 2 * odd], {"col": far}))

    def arrival(k):
        return pltpu.make_async_copy(ao_ref.at[k], ao_ref.at[k], a_recv.at[k])

    for d in range(1, rows):
        for h in range(2):
            above = lax.rem(2 * (r + d) + h, panels)
            has_above = (r + d <= rows - 1) & carried(above, 0, r)

            @pl.when(has_above)
            def _():
                arrival(above).wait()
            if d < rows - 1:
                a_pair(above, h, d, ao_ref.at[above])[0](has_above)
            below = lax.rem(2 * (r - d) + h + 2 * panels, panels)
            has_below = (r - d >= 0) & carried(below, r, rows - 1)

            @pl.when(has_below)
            def _():
                arrival(below).wait()
            if d < rows - 1:
                a_pair(below, h, d, ao_ref.at[below])[1](has_below)

    parity = lax.rem(p, 2)
    partner = p + 1 - 2 * parity

    def b_arrival(h, s):
        return pltpu.make_async_copy(bo_ref.at[h, s], bo_ref.at[h, s], b_recv.at[h, s])

    for h in range(2):
        home = lax.rem(p + 2 * r + h + 1, cols)

        @pl.when(home != p)
        def _():
            b_arrival(h, 1).wait()
        to_slot = 2 * parity
        for own_it in range(2):
            src = b_ref.at[h] if own_it else bo_ref.at[h, 1]
            here = (home == p) if own_it else ((home != p) & (home != partner))
            go(here, remote(src, bo_ref.at[h, to_slot], b_pass.at[h, own_it], b_recv.at[h, to_slot],
                            {"col": partner}))
    for h in range(2):
        for s in (0, 2):
            home = lax.rem(p + 2 * r + h + s, cols)

            @pl.when(home != p)
            def _():
                b_arrival(h, s).wait()
    for d in range(1, rows):
        pltpu.make_async_copy(ai_ref, aio_ref.at[0], ai_recv.at[d]).wait()
    for j in range(span):
        home = lax.rem(p + 2 * r + j, cols)

        @pl.when(home != p)
        def _():
            pltpu.make_async_copy(bi_ref, bio_ref.at[j], bi_recv.at[j]).wait()
    own_a.wait()
    for cond, copy in sends:
        @pl.when(cond)
        def _():
            copy.wait_send()


def multiply_kernel(rows, cols, steps, pairs_ref, count_ref, aid_ref, bid_ref, a_ref, ao_ref, b_ref, bo_ref, c_ref,
                    a_vm, b_vm, acc, out_vm, a_sem, b_sem, c_sem):
    p = lax.axis_index("col")
    r = lax.axis_index("row")
    panels = 2 * rows
    edge = acc.shape[-1]

    def load_a(j, act):
        k = lax.rem(p + 2 * r + j, panels)
        h = lax.rem(k, 2)

        @pl.when(k // 2 == r)
        def _():
            act(pltpu.make_async_copy(a_ref.at[h], a_vm.at[j], a_sem.at[j]))

        @pl.when(k // 2 != r)
        def _():
            act(pltpu.make_async_copy(ao_ref.at[k], a_vm.at[j], a_sem.at[j]))

    def load_b(h, s, act):
        k = lax.rem(p + 2 * r + h + s, cols)

        @pl.when(k == p)
        def _():
            act(pltpu.make_async_copy(b_ref.at[h], b_vm.at[h, s], b_sem.at[h, s]))

        @pl.when(k != p)
        def _():
            act(pltpu.make_async_copy(bo_ref.at[h, s], b_vm.at[h, s], b_sem.at[h, s]))

    start = lambda copy: copy.start()
    wait = lambda copy: copy.wait()
    for h in range(2):
        for s in range(steps):
            if h == 0 or s == steps - 1:
                load_a(h + s, start)
            load_b(h, s, start)
    outs = []
    for h in range(2):
        @pl.loop(0, WB * WB)
        def _(t):
            acc[t] = jnp.zeros(acc.shape[1:], acc.dtype)
        for s in range(steps):
            j = h + s
            if h == 0 or s == steps - 1:
                load_a(j, wait)
            load_b(h, s, wait)
            k = lax.rem(p + 2 * r + j, panels)

            def one(i):
                a = pairs_ref[h, s, 0, i]
                b = pairs_ref[h, s, 1, i]
                t = lax.rem(aid_ref[k, a], WB) * WB + lax.rem(bid_ref[2 * j + h, b], WB)
                return t, jnp.dot(a_vm[j, a], b_vm[h, s, b], preferred_element_type=jnp.float32)

            count = count_ref[h, s]

            @pl.loop(0, count // 2)
            def _(i):
                t0, v0 = one(2 * i)
                t1, v1 = one(2 * i + 1)
                acc[t0] += v0
                acc[t1] += v1

            @pl.when(lax.rem(count, 2) == 1)
            def _():
                t0, v0 = one(count - 1)
                acc[t0] += v0
        for row in range(WB):
            for col in range(WB):
                out_vm[h, row, :, col * edge:(col + 1) * edge] = acc[row * WB + col].astype(out_vm.dtype)
            copy = pltpu.make_async_copy(
                out_vm.at[h, row],
                c_ref.at[pl.ds(row * edge, edge), pl.ds(h * WB * edge, WB * edge)],
                c_sem.at[h, row])
            copy.start()
            outs.append(copy)
    for copy in outs:
        copy.wait()


def body(rows, cols, a_blocks, a_index, b_blocks, b_index, pair_list, pair_count):
    a, b = a_blocks[0], b_blocks[0]
    cap, edge = a.shape[1], a.shape[-1]
    steps = pair_list.shape[2]
    panel = (cap, edge, edge)
    dma = pltpu.SemaphoreType.DMA
    sds = jax.ShapeDtypeStruct
    ao, aio, bo, bio = pl.pallas_call(
        functools.partial(move_kernel, rows, cols, steps),
        out_shape=(
            sds((2 * rows,) + panel, a.dtype),
            sds((rows, 2, cap), jnp.int32),
            sds((2, steps) + panel, b.dtype),
            sds((steps + 1, 2, cap), jnp.int32),
        ),
        in_specs=[ANY] * 4,
        out_specs=(ANY,) * 4,
        scratch_shapes=[
            dma((2 * rows,)), dma((rows, 2)), dma((rows, 2)), dma((rows,)), dma((rows,)),
            dma((2, steps)), dma((2, 2)), dma((2, 2)), dma((steps + 1,)), dma((steps + 1,)), dma((2,)),
        ],
        compiler_params=pltpu.CompilerParams(has_side_effects=True),
        name="move",
    )(a, a_index[0], b, b_index[0])
    return pl.pallas_call(
        functools.partial(multiply_kernel, rows, cols, steps),
        out_shape=sds((WB * edge, 2 * WB * edge), jnp.bfloat16),
        in_specs=[SMEM] * 4 + [ANY] * 4,
        out_specs=ANY,
        scratch_shapes=[
            pltpu.VMEM((steps + 1,) + panel, a.dtype),
            pltpu.VMEM((2, steps) + panel, b.dtype),
            pltpu.VMEM((WB * WB, edge, edge), jnp.float32),
            pltpu.VMEM((2, WB, edge, WB * edge), jnp.bfloat16),
            dma((steps + 1,)), dma((2, steps)), dma((2, WB)),
        ],
        compiler_params=pltpu.CompilerParams(vmem_limit_bytes=60000 * 1024),
        name="multiply",
    )(pair_list[0], pair_count[0], aio.reshape(2 * rows, cap), bio.reshape(2 * (steps + 1), cap), a, ao, b, bo)


def solution(mesh):
    in_specs = (
        P("col", "row", None, None, None),
        P("col", "row", None),
        P("col", "row", None, None, None),
        P("col", "row", None),
        P("col", "row", None, None, None),
        P("col", "row", None),
    )
    return jax.shard_map(
        functools.partial(body, mesh.shape["row"], mesh.shape["col"]),
        mesh=mesh, in_specs=in_specs, out_specs=P("col", "row"), check_vma=False)
```

```python
import functools

import jax
import jax.numpy as jnp
from jax import lax
from jax.experimental import pallas as pl
from jax.experimental.pallas import tpu as pltpu
from jax.sharding import PartitionSpec as P

WB = 10
CHUNKS = 4
MESH = pl.DeviceIdType.MESH
ANY = pl.BlockSpec(memory_space=pl.ANY)
SMEM = pl.BlockSpec(memory_space=pltpu.SMEM)


def move_kernel(rows, cols, steps, a_ref, ai_ref, b_ref, bi_ref, ao_ref, aio_ref, bo_ref, bio_ref,
                a_recv, a_down, a_up, ai_recv, ai_send, b_recv, b_send, b_pass, bi_recv, bi_send, own):
    p = lax.axis_index("col")
    r = lax.axis_index("row")
    panels = 2 * rows
    span = steps + 1
    cap = a_ref.shape[1]
    sends = []

    def remote(src, dst, send_sem, recv_sem, device):
        return pltpu.make_async_remote_copy(
            src_ref=src, dst_ref=dst, send_sem=send_sem, recv_sem=recv_sem,
            device_id=device, device_id_type=MESH)

    def go(cond, copy):
        @pl.when(cond)
        def _():
            copy.start()
        sends.append((cond, copy))

    def needed(k, row):
        return lax.rem(k - p - 2 * row + 2 * panels + cols, panels) < span

    def carried(k, lo, hi):
        total = 0
        for row in range(rows):
            hit = needed(k, row) & (row >= lo) & (row <= hi)
            total = total + jnp.where(hit, 1, 0)
        return total > 0

    own_a = pltpu.make_async_copy(ai_ref, aio_ref.at[r], own.at[0])
    own_a.start()
    for d in range(1, rows):
        to = lax.rem(r + d, rows)
        go(r >= 0, remote(ai_ref, aio_ref.at[r], ai_send.at[d], ai_recv.at[d], {"row": to}))
    own_slot = lax.rem(2 * cols - 2 * r, cols)
    for j in range(span):
        to = lax.rem(p - 2 * r - j + 2 * cols, cols)
        go(to != p, remote(bi_ref, bio_ref.at[j], bi_send.at[j], bi_recv.at[j], {"col": to}))

        @pl.when(own_slot == j)
        def _():
            keep = pltpu.make_async_copy(bi_ref, bio_ref.at[j], own.at[1])
            keep.start()
            keep.wait()

    cuts = [cap * i // CHUNKS for i in range(CHUNKS + 1)]
    pieces = [pl.ds(cuts[i], cuts[i + 1] - cuts[i]) for i in range(CHUNKS)]

    def down_cond(k):
        return (r >= 1) & carried(k, 0, r - 1)

    def up_cond(k):
        return (r <= rows - 2) & carried(k, r + 1, rows - 1)

    def hop(src, k, c, send_sem, to):
        return remote(src.at[pieces[c]], ao_ref.at[k, pieces[c]], send_sem.at[c], a_recv.at[k, c], {"row": to})

    def down_hop(src, k, h, d, c):
        return hop(src, k, c, a_down.at[d, h], lax.max(r - 1, 0))

    def up_hop(src, k, h, d, c):
        return hop(src, k, c, a_up.at[d, h], lax.min(r + 1, rows - 1))

    for h in range(2):
        k = 2 * r + h
        for c in range(CHUNKS):
            go(down_cond(k), down_hop(a_ref.at[h], k, h, 0, c))
            go(up_cond(k), up_hop(a_ref.at[h], k, h, 0, c))
    for h in range(2):
        base = lax.rem(p - 2 * r - h + 2 * cols, cols)
        near = lax.rem(base - 1 + cols, cols)
        odd = lax.rem(base, 2)
        far = lax.rem(base - 2 * odd + cols, cols)
        go(near != p, remote(b_ref.at[h], bo_ref.at[h, 1], b_send.at[h, 0], b_recv.at[h, 1], {"col": near}))
        go(far != p, remote(b_ref.at[h], bo_ref.at[h, 2 * odd], b_send.at[h, 1], b_recv.at[h, 2 * odd], {"col": far}))

    def arrival(k, c):
        ref = ao_ref.at[k, pieces[c]]
        return pltpu.make_async_copy(ref, ref, a_recv.at[k, c])

    rest = []
    for d in range(1, rows):
        for h in range(2):
            above = lax.rem(2 * (r + d) + h, panels)
            below = lax.rem(2 * (r - d) + h + 2 * panels, panels)
            has_above = (r + d <= rows - 1) & carried(above, 0, r)
            has_below = (r - d >= 0) & carried(below, r, rows - 1)
            on_down = has_above & down_cond(above)
            on_up = has_below & up_cond(below)
            for c in range(CHUNKS):
                for on, k, hop_to in ((on_down, above, down_hop), (on_up, below, up_hop)):
                    if d < rows - 1:
                        @pl.when(on)
                        def _():
                            arrival(k, c).wait()
                        go(on, hop_to(ao_ref.at[k], k, h, d, c))
            for on, has, k in ((on_down, has_above, above), (on_up, has_below, below)):
                rest.append((has & jnp.logical_not(on) if d < rows - 1 else has, k))

    parity = lax.rem(p, 2)
    partner = p + 1 - 2 * parity

    def b_arrival(h, s):
        return pltpu.make_async_copy(bo_ref.at[h, s], bo_ref.at[h, s], b_recv.at[h, s])

    for h in range(2):
        home = lax.rem(p + 2 * r + h + 1, cols)

        @pl.when(home != p)
        def _():
            b_arrival(h, 1).wait()
        to_slot = 2 * parity
        for own_it in range(2):
            src = b_ref.at[h] if own_it else bo_ref.at[h, 1]
            here = (home == p) if own_it else ((home != p) & (home != partner))
            go(here, remote(src, bo_ref.at[h, to_slot], b_pass.at[h, own_it], b_recv.at[h, to_slot],
                            {"col": partner}))
    for h in range(2):
        for s in (0, 2):
            home = lax.rem(p + 2 * r + h + s, cols)

            @pl.when(home != p)
            def _():
                b_arrival(h, s).wait()
    for has, k in rest:
        @pl.when(has)
        def _():
            for c in range(CHUNKS):
                arrival(k, c).wait()
    for d in range(1, rows):
        pltpu.make_async_copy(ai_ref, aio_ref.at[0], ai_recv.at[d]).wait()
    for j in range(span):
        home = lax.rem(p + 2 * r + j, cols)

        @pl.when(home != p)
        def _():
            pltpu.make_async_copy(bi_ref, bio_ref.at[j], bi_recv.at[j]).wait()
    own_a.wait()
    for cond, copy in sends:
        @pl.when(cond)
        def _():
            copy.wait_send()


def multiply_kernel(rows, cols, steps, pairs_ref, count_ref, aid_ref, bid_ref, a_ref, ao_ref, b_ref, bo_ref, c_ref,
                    a_vm, b_vm, acc, out_vm, a_sem, b_sem, c_sem):
    p = lax.axis_index("col")
    r = lax.axis_index("row")
    panels = 2 * rows
    edge = acc.shape[-1]

    def load_a(j, act):
        k = lax.rem(p + 2 * r + j, panels)
        h = lax.rem(k, 2)

        @pl.when(k // 2 == r)
        def _():
            act(pltpu.make_async_copy(a_ref.at[h], a_vm.at[j], a_sem.at[j]))

        @pl.when(k // 2 != r)
        def _():
            act(pltpu.make_async_copy(ao_ref.at[k], a_vm.at[j], a_sem.at[j]))

    def load_b(h, s, act):
        k = lax.rem(p + 2 * r + h + s, cols)

        @pl.when(k == p)
        def _():
            act(pltpu.make_async_copy(b_ref.at[h], b_vm.at[h, s], b_sem.at[h, s]))

        @pl.when(k != p)
        def _():
            act(pltpu.make_async_copy(bo_ref.at[h, s], b_vm.at[h, s], b_sem.at[h, s]))

    start = lambda copy: copy.start()
    wait = lambda copy: copy.wait()
    for h in range(2):
        for s in range(steps):
            if h == 0 or s == steps - 1:
                load_a(h + s, start)
            load_b(h, s, start)
    outs = []
    for h in range(2):
        @pl.loop(0, WB * WB)
        def _(t):
            acc[t] = jnp.zeros(acc.shape[1:], acc.dtype)
        for s in range(steps):
            j = h + s
            if h == 0 or s == steps - 1:
                load_a(j, wait)
            load_b(h, s, wait)
            k = lax.rem(p + 2 * r + j, panels)

            def one(i):
                a = pairs_ref[h, s, 0, i]
                b = pairs_ref[h, s, 1, i]
                t = lax.rem(aid_ref[k, a], WB) * WB + lax.rem(bid_ref[2 * j + h, b], WB)
                return t, jnp.dot(a_vm[j, a], b_vm[h, s, b], preferred_element_type=jnp.float32)

            count = count_ref[h, s]

            @pl.loop(0, count // 2)
            def _(i):
                t0, v0 = one(2 * i)
                t1, v1 = one(2 * i + 1)
                acc[t0] += v0
                acc[t1] += v1

            @pl.when(lax.rem(count, 2) == 1)
            def _():
                t0, v0 = one(count - 1)
                acc[t0] += v0
        for row in range(WB):
            for col in range(WB):
                out_vm[h, row, :, col * edge:(col + 1) * edge] = acc[row * WB + col].astype(out_vm.dtype)
            copy = pltpu.make_async_copy(
                out_vm.at[h, row],
                c_ref.at[pl.ds(row * edge, edge), pl.ds(h * WB * edge, WB * edge)],
                c_sem.at[h, row])
            copy.start()
            outs.append(copy)
    for copy in outs:
        copy.wait()


def body(rows, cols, a_blocks, a_index, b_blocks, b_index, pair_list, pair_count):
    a, b = a_blocks[0], b_blocks[0]
    cap, edge = a.shape[1], a.shape[-1]
    steps = pair_list.shape[2]
    panel = (cap, edge, edge)
    dma = pltpu.SemaphoreType.DMA
    sds = jax.ShapeDtypeStruct
    ao, aio, bo, bio = pl.pallas_call(
        functools.partial(move_kernel, rows, cols, steps),
        out_shape=(
            sds((2 * rows,) + panel, a.dtype),
            sds((rows, 2, cap), jnp.int32),
            sds((2, steps) + panel, b.dtype),
            sds((steps + 1, 2, cap), jnp.int32),
        ),
        in_specs=[ANY] * 4,
        out_specs=(ANY,) * 4,
        scratch_shapes=[
            dma((2 * rows, CHUNKS)), dma((rows, 2, CHUNKS)), dma((rows, 2, CHUNKS)), dma((rows,)), dma((rows,)),
            dma((2, steps)), dma((2, 2)), dma((2, 2)), dma((steps + 1,)), dma((steps + 1,)), dma((2,)),
        ],
        compiler_params=pltpu.CompilerParams(has_side_effects=True),
        name="move",
    )(a, a_index[0], b, b_index[0])
    return pl.pallas_call(
        functools.partial(multiply_kernel, rows, cols, steps),
        out_shape=sds((WB * edge, 2 * WB * edge), jnp.bfloat16),
        in_specs=[SMEM] * 4 + [ANY] * 4,
        out_specs=ANY,
        scratch_shapes=[
            pltpu.VMEM((steps + 1,) + panel, a.dtype),
            pltpu.VMEM((2, steps) + panel, b.dtype),
            pltpu.VMEM((WB * WB, edge, edge), jnp.float32),
            pltpu.VMEM((2, WB, edge, WB * edge), jnp.bfloat16),
            dma((steps + 1,)), dma((2, steps)), dma((2, WB)),
        ],
        compiler_params=pltpu.CompilerParams(vmem_limit_bytes=60000 * 1024),
        name="multiply",
    )(pair_list[0], pair_count[0], aio.reshape(2 * rows, cap), bio.reshape(2 * (steps + 1), cap), a, ao, b, bo)


def solution(mesh):
    in_specs = (
        P("col", "row", None, None, None),
        P("col", "row", None),
        P("col", "row", None, None, None),
        P("col", "row", None),
        P("col", "row", None, None, None),
        P("col", "row", None),
    )
    return jax.shard_map(
        functools.partial(body, mesh.shape["row"], mesh.shape["col"]),
        mesh=mesh, in_specs=in_specs, out_specs=P("col", "row"), check_vma=False)
```

```python
import functools

import jax
import jax.numpy as jnp
from jax import lax
from jax.experimental import pallas as pl
from jax.experimental.pallas import tpu as pltpu
from jax.sharding import PartitionSpec as P

WB = 10
CHUNKS = 4
MESH = pl.DeviceIdType.MESH
ANY = pl.BlockSpec(memory_space=pl.ANY)
SMEM = pl.BlockSpec(memory_space=pltpu.SMEM)


def move_kernel(rows, cols, steps, a_ref, ai_ref, b_ref, bi_ref, ao_ref, aio_ref, bo_ref, bio_ref, via_ref,
                a_recv, a_down, a_up, ai_recv, ai_send, b_recv, b_send, b_pass, bi_recv, bi_send, own, v_recv, v_send):
    p = lax.axis_index("col")
    r = lax.axis_index("row")
    panels = 2 * rows
    span = steps + 1
    cap = a_ref.shape[1]
    sends = []

    def remote(src, dst, send_sem, recv_sem, device):
        return pltpu.make_async_remote_copy(
            src_ref=src, dst_ref=dst, send_sem=send_sem, recv_sem=recv_sem,
            device_id=device, device_id_type=MESH)

    def go(cond, copy):
        @pl.when(cond)
        def _():
            copy.start()
        sends.append((cond, copy))

    def needed(k, row, line=p):
        return lax.rem(k - line - 2 * row + 2 * panels + cols, panels) < span

    def detours(line, home, h, way):
        k = 2 * home + h
        near, others = 0, 0
        for row in range(rows):
            ahead = (row - home) * way
            hit = needed(k, row, line) & (ahead > 0)
            near = near + jnp.where(hit & (ahead == 2), 1, 0)
            others = others + jnp.where(hit & (ahead != 2), 1, 0)
        inside = (home >= 0) & (home <= rows - 1)
        turn = (lax.rem(line, 2) == 1) & (lax.rem((line + 2) // 4, 2) == 1)
        return inside & turn & (near == 1) & (others == 0)

    beside = p + 2 - 4 * lax.rem(p // 2, 2)

    def carried(k, lo, hi):
        total = 0
        for row in range(rows):
            hit = needed(k, row) & (row >= lo) & (row <= hi)
            total = total + jnp.where(hit, 1, 0)
        return total > 0

    own_a = pltpu.make_async_copy(ai_ref, aio_ref.at[r], own.at[0])
    own_a.start()
    for d in range(1, rows):
        to = lax.rem(r + d, rows)
        go(r >= 0, remote(ai_ref, aio_ref.at[r], ai_send.at[d], ai_recv.at[d], {"row": to}))
    own_slot = lax.rem(2 * cols - 2 * r, cols)
    for j in range(span):
        to = lax.rem(p - 2 * r - j + 2 * cols, cols)
        go(to != p, remote(bi_ref, bio_ref.at[j], bi_send.at[j], bi_recv.at[j], {"col": to}))

        @pl.when(own_slot == j)
        def _():
            keep = pltpu.make_async_copy(bi_ref, bio_ref.at[j], own.at[1])
            keep.start()
            keep.wait()

    cuts = [cap * i // CHUNKS for i in range(CHUNKS + 1)]
    pieces = [pl.ds(cuts[i], cuts[i + 1] - cuts[i]) for i in range(CHUNKS)]

    def down_cond(k):
        return (r >= 1) & carried(k, 0, r - 1) & jnp.logical_not(detours(p, k // 2, lax.rem(k, 2), -1))

    def up_cond(k):
        return (r <= rows - 2) & carried(k, r + 1, rows - 1) & jnp.logical_not(detours(p, k // 2, lax.rem(k, 2), 1))

    def hop(src, k, c, send_sem, to):
        return remote(src.at[pieces[c]], ao_ref.at[k, pieces[c]], send_sem.at[c], a_recv.at[k, c], {"row": to})

    def down_hop(src, k, h, d, c):
        return hop(src, k, c, a_down.at[d, h], lax.max(r - 1, 0))

    def up_hop(src, k, h, d, c):
        return hop(src, k, c, a_up.at[d, h], lax.min(r + 1, rows - 1))

    for h in range(2):
        k = 2 * r + h
        for c in range(CHUNKS):
            go(down_cond(k), down_hop(a_ref.at[h], k, h, 0, c))
            go(up_cond(k), up_hop(a_ref.at[h], k, h, 0, c))
    for h in range(2):
        for i, way in enumerate((-1, 1)):
            leaves = detours(p, r, h, way)
            for c in range(CHUNKS):
                go(leaves, remote(a_ref.at[h, pieces[c]], via_ref.at[i, 0, pieces[c]],
                                  v_send.at[i, h, c], v_recv.at[i, 0, c], {"col": beside}))

    def via_arrival(i, leg, c):
        ref = via_ref.at[i, leg, pieces[c]]
        return pltpu.make_async_copy(ref, ref, v_recv.at[i, leg, c])

    def via_along():
        for i, way in enumerate((-1, 1)):
            on = detours(beside, r, 0, way) | detours(beside, r, 1, way)
            to = lax.rem(r + 2 * way + 2 * rows, rows)
            for c in range(CHUNKS):
                @pl.when(on)
                def _():
                    via_arrival(i, 0, c).wait()
                go(on, remote(via_ref.at[i, 0, pieces[c]], via_ref.at[i, 1, pieces[c]],
                              v_send.at[i, 2, c], v_recv.at[i, 1, c], {"row": to}))

    def via_back():
        for i, way in enumerate((-1, 1)):
            home = r - 2 * way
            second = detours(beside, home, 1, way)
            on = detours(beside, home, 0, way) | second
            k = lax.rem(2 * home + jnp.where(second, 1, 0) + 2 * panels, panels)
            for c in range(CHUNKS):
                @pl.when(on)
                def _():
                    via_arrival(i, 1, c).wait()
                go(on, remote(via_ref.at[i, 1, pieces[c]], ao_ref.at[k, pieces[c]],
                              v_send.at[i, 3, c], a_recv.at[k, c], {"col": beside}))
    for h in range(2):
        base = lax.rem(p - 2 * r - h + 2 * cols, cols)
        near = lax.rem(base - 1 + cols, cols)
        odd = lax.rem(base, 2)
        far = lax.rem(base - 2 * odd + cols, cols)
        go(near != p, remote(b_ref.at[h], bo_ref.at[h, 1], b_send.at[h, 0], b_recv.at[h, 1], {"col": near}))
        go(far != p, remote(b_ref.at[h], bo_ref.at[h, 2 * odd], b_send.at[h, 1], b_recv.at[h, 2 * odd], {"col": far}))

    def arrival(k, c):
        ref = ao_ref.at[k, pieces[c]]
        return pltpu.make_async_copy(ref, ref, a_recv.at[k, c])

    rest = []
    for d in range(1, rows):
        for h in range(2):
            above = lax.rem(2 * (r + d) + h, panels)
            below = lax.rem(2 * (r - d) + h + 2 * panels, panels)
            has_above = (r + d <= rows - 1) & carried(above, 0, r)
            has_below = (r - d >= 0) & carried(below, r, rows - 1)
            if d != 2:
                has_above = has_above & jnp.logical_not(detours(p, r + d, h, -1))
                has_below = has_below & jnp.logical_not(detours(p, r - d, h, 1))
            on_down = has_above & down_cond(above)
            on_up = has_below & up_cond(below)
            for c in range(CHUNKS):
                for on, k, hop_to in ((on_down, above, down_hop), (on_up, below, up_hop)):
                    if d < rows - 1:
                        @pl.when(on)
                        def _():
                            arrival(k, c).wait()
                        go(on, hop_to(ao_ref.at[k], k, h, d, c))
            for on, has, k in ((on_down, has_above, above), (on_up, has_below, below)):
                rest.append((has & jnp.logical_not(on) if d < rows - 1 else has, k))
        if d == 1:
            via_along()
    via_back()

    parity = lax.rem(p, 2)
    partner = p + 1 - 2 * parity

    def b_arrival(h, s):
        return pltpu.make_async_copy(bo_ref.at[h, s], bo_ref.at[h, s], b_recv.at[h, s])

    for h in range(2):
        home = lax.rem(p + 2 * r + h + 1, cols)

        @pl.when(home != p)
        def _():
            b_arrival(h, 1).wait()
        to_slot = 2 * parity
        for own_it in range(2):
            src = b_ref.at[h] if own_it else bo_ref.at[h, 1]
            here = (home == p) if own_it else ((home != p) & (home != partner))
            go(here, remote(src, bo_ref.at[h, to_slot], b_pass.at[h, own_it], b_recv.at[h, to_slot],
                            {"col": partner}))
    for h in range(2):
        for s in (0, 2):
            home = lax.rem(p + 2 * r + h + s, cols)

            @pl.when(home != p)
            def _():
                b_arrival(h, s).wait()
    for has, k in rest:
        @pl.when(has)
        def _():
            for c in range(CHUNKS):
                arrival(k, c).wait()
    for d in range(1, rows):
        pltpu.make_async_copy(ai_ref, aio_ref.at[0], ai_recv.at[d]).wait()
    for j in range(span):
        home = lax.rem(p + 2 * r + j, cols)

        @pl.when(home != p)
        def _():
            pltpu.make_async_copy(bi_ref, bio_ref.at[j], bi_recv.at[j]).wait()
    own_a.wait()
    for cond, copy in sends:
        @pl.when(cond)
        def _():
            copy.wait_send()


def multiply_kernel(rows, cols, steps, pairs_ref, count_ref, aid_ref, bid_ref, a_ref, ao_ref, b_ref, bo_ref, c_ref,
                    a_vm, b_vm, acc, out_vm, a_sem, b_sem, c_sem):
    p = lax.axis_index("col")
    r = lax.axis_index("row")
    panels = 2 * rows
    edge = acc.shape[-1]

    def load_a(j, act):
        k = lax.rem(p + 2 * r + j, panels)
        h = lax.rem(k, 2)

        @pl.when(k // 2 == r)
        def _():
            act(pltpu.make_async_copy(a_ref.at[h], a_vm.at[j], a_sem.at[j]))

        @pl.when(k // 2 != r)
        def _():
            act(pltpu.make_async_copy(ao_ref.at[k], a_vm.at[j], a_sem.at[j]))

    def load_b(h, s, act):
        k = lax.rem(p + 2 * r + h + s, cols)

        @pl.when(k == p)
        def _():
            act(pltpu.make_async_copy(b_ref.at[h], b_vm.at[h, s], b_sem.at[h, s]))

        @pl.when(k != p)
        def _():
            act(pltpu.make_async_copy(bo_ref.at[h, s], b_vm.at[h, s], b_sem.at[h, s]))

    start = lambda copy: copy.start()
    wait = lambda copy: copy.wait()
    for h in range(2):
        for s in range(steps):
            if h == 0 or s == steps - 1:
                load_a(h + s, start)
            load_b(h, s, start)
    outs = []
    for h in range(2):
        @pl.loop(0, WB * WB)
        def _(t):
            acc[t] = jnp.zeros(acc.shape[1:], acc.dtype)
        for s in range(steps):
            j = h + s
            if h == 0 or s == steps - 1:
                load_a(j, wait)
            load_b(h, s, wait)
            k = lax.rem(p + 2 * r + j, panels)

            def one(i):
                a = pairs_ref[h, s, 0, i]
                b = pairs_ref[h, s, 1, i]
                t = lax.rem(aid_ref[k, a], WB) * WB + lax.rem(bid_ref[2 * j + h, b], WB)
                return t, jnp.dot(a_vm[j, a], b_vm[h, s, b], preferred_element_type=jnp.float32)

            count = count_ref[h, s]

            @pl.loop(0, count // 2)
            def _(i):
                t0, v0 = one(2 * i)
                t1, v1 = one(2 * i + 1)
                acc[t0] += v0
                acc[t1] += v1

            @pl.when(lax.rem(count, 2) == 1)
            def _():
                t0, v0 = one(count - 1)
                acc[t0] += v0
        for row in range(WB):
            for col in range(WB):
                out_vm[h, row, :, col * edge:(col + 1) * edge] = acc[row * WB + col].astype(out_vm.dtype)
            copy = pltpu.make_async_copy(
                out_vm.at[h, row],
                c_ref.at[pl.ds(row * edge, edge), pl.ds(h * WB * edge, WB * edge)],
                c_sem.at[h, row])
            copy.start()
            outs.append(copy)
    for copy in outs:
        copy.wait()


def body(rows, cols, a_blocks, a_index, b_blocks, b_index, pair_list, pair_count):
    a, b = a_blocks[0], b_blocks[0]
    cap, edge = a.shape[1], a.shape[-1]
    steps = pair_list.shape[2]
    panel = (cap, edge, edge)
    dma = pltpu.SemaphoreType.DMA
    sds = jax.ShapeDtypeStruct
    ao, aio, bo, bio, _ = pl.pallas_call(
        functools.partial(move_kernel, rows, cols, steps),
        out_shape=(
            sds((2 * rows,) + panel, a.dtype),
            sds((rows, 2, cap), jnp.int32),
            sds((2, steps) + panel, b.dtype),
            sds((steps + 1, 2, cap), jnp.int32),
            sds((2, 2) + panel, a.dtype),
        ),
        in_specs=[ANY] * 4,
        out_specs=(ANY,) * 5,
        scratch_shapes=[
            dma((2 * rows, CHUNKS)), dma((rows, 2, CHUNKS)), dma((rows, 2, CHUNKS)), dma((rows,)), dma((rows,)),
            dma((2, steps)), dma((2, 2)), dma((2, 2)), dma((steps + 1,)), dma((steps + 1,)), dma((2,)),
            dma((2, 2, CHUNKS)), dma((2, 4, CHUNKS)),
        ],
        compiler_params=pltpu.CompilerParams(has_side_effects=True),
        name="move",
    )(a, a_index[0], b, b_index[0])
    return pl.pallas_call(
        functools.partial(multiply_kernel, rows, cols, steps),
        out_shape=sds((WB * edge, 2 * WB * edge), jnp.bfloat16),
        in_specs=[SMEM] * 4 + [ANY] * 4,
        out_specs=ANY,
        scratch_shapes=[
            pltpu.VMEM((steps + 1,) + panel, a.dtype),
            pltpu.VMEM((2, steps) + panel, b.dtype),
            pltpu.VMEM((WB * WB, edge, edge), jnp.float32),
            pltpu.VMEM((2, WB, edge, WB * edge), jnp.bfloat16),
            dma((steps + 1,)), dma((2, steps)), dma((2, WB)),
        ],
        compiler_params=pltpu.CompilerParams(vmem_limit_bytes=60000 * 1024),
        name="multiply",
    )(pair_list[0], pair_count[0], aio.reshape(2 * rows, cap), bio.reshape(2 * (steps + 1), cap), a, ao, b, bo)


def solution(mesh):
    in_specs = (
        P("col", "row", None, None, None),
        P("col", "row", None),
        P("col", "row", None, None, None),
        P("col", "row", None),
        P("col", "row", None, None, None),
        P("col", "row", None),
    )
    return jax.shard_map(
        functools.partial(body, mesh.shape["row"], mesh.shape["col"]),
        mesh=mesh, in_specs=in_specs, out_specs=P("col", "row"), check_vma=False)
```

```python
import functools

import jax
import jax.numpy as jnp
from jax import lax
from jax.experimental import pallas as pl
from jax.experimental.pallas import tpu as pltpu
from jax.sharding import PartitionSpec as P

WB = 10
CHUNKS = 4
UNROLL = 4
MESH = pl.DeviceIdType.MESH
ANY = pl.BlockSpec(memory_space=pl.ANY)
SMEM = pl.BlockSpec(memory_space=pltpu.SMEM)


def move_kernel(rows, cols, steps, a_ref, ai_ref, b_ref, bi_ref, ao_ref, aio_ref, bo_ref, bio_ref, via_ref,
                a_recv, a_down, a_up, ai_recv, ai_send, b_recv, b_send, b_pass, bi_recv, bi_send, own, v_recv, v_send):
    p = lax.axis_index("col")
    r = lax.axis_index("row")
    panels = 2 * rows
    span = steps + 1
    cap = a_ref.shape[1]
    sends = []

    def remote(src, dst, send_sem, recv_sem, device):
        return pltpu.make_async_remote_copy(
            src_ref=src, dst_ref=dst, send_sem=send_sem, recv_sem=recv_sem,
            device_id=device, device_id_type=MESH)

    def go(cond, copy):
        @pl.when(cond)
        def _():
            copy.start()
        sends.append((cond, copy))

    def needed(k, row, line=p):
        return lax.rem(k - line - 2 * row + 2 * panels + cols, panels) < span

    def detours(line, home, h, way):
        k = 2 * home + h
        near, others = 0, 0
        for row in range(rows):
            ahead = (row - home) * way
            hit = needed(k, row, line) & (ahead > 0)
            near = near + jnp.where(hit & (ahead == 2), 1, 0)
            others = others + jnp.where(hit & (ahead != 2), 1, 0)
        inside = (home >= 0) & (home <= rows - 1)
        turn = (lax.rem(line, 2) == 1) & (lax.rem((line + 2) // 4, 2) == 1)
        return inside & turn & (near == 1) & (others == 0)

    beside = p + 2 - 4 * lax.rem(p // 2, 2)

    def carried(k, lo, hi):
        total = 0
        for row in range(rows):
            hit = needed(k, row) & (row >= lo) & (row <= hi)
            total = total + jnp.where(hit, 1, 0)
        return total > 0

    own_a = pltpu.make_async_copy(ai_ref, aio_ref.at[r], own.at[0])
    own_a.start()
    for d in range(1, rows):
        to = lax.rem(r + d, rows)
        go(r >= 0, remote(ai_ref, aio_ref.at[r], ai_send.at[d], ai_recv.at[d], {"row": to}))
    own_slot = lax.rem(2 * cols - 2 * r, cols)
    for j in range(span):
        to = lax.rem(p - 2 * r - j + 2 * cols, cols)
        go(to != p, remote(bi_ref, bio_ref.at[j], bi_send.at[j], bi_recv.at[j], {"col": to}))

        @pl.when(own_slot == j)
        def _():
            keep = pltpu.make_async_copy(bi_ref, bio_ref.at[j], own.at[1])
            keep.start()
            keep.wait()

    cuts = [cap * i // CHUNKS for i in range(CHUNKS + 1)]
    pieces = [pl.ds(cuts[i], cuts[i + 1] - cuts[i]) for i in range(CHUNKS)]

    def down_cond(k):
        return (r >= 1) & carried(k, 0, r - 1) & jnp.logical_not(detours(p, k // 2, lax.rem(k, 2), -1))

    def up_cond(k):
        return (r <= rows - 2) & carried(k, r + 1, rows - 1) & jnp.logical_not(detours(p, k // 2, lax.rem(k, 2), 1))

    def hop(src, k, c, send_sem, to):
        return remote(src.at[pieces[c]], ao_ref.at[k, pieces[c]], send_sem.at[c], a_recv.at[k, c], {"row": to})

    def down_hop(src, k, h, d, c):
        return hop(src, k, c, a_down.at[d, h], lax.max(r - 1, 0))

    def up_hop(src, k, h, d, c):
        return hop(src, k, c, a_up.at[d, h], lax.min(r + 1, rows - 1))

    for h in range(2):
        k = 2 * r + h
        for c in range(CHUNKS):
            go(down_cond(k), down_hop(a_ref.at[h], k, h, 0, c))
            go(up_cond(k), up_hop(a_ref.at[h], k, h, 0, c))
    for h in range(2):
        for i, way in enumerate((-1, 1)):
            leaves = detours(p, r, h, way)
            for c in range(CHUNKS):
                go(leaves, remote(a_ref.at[h, pieces[c]], via_ref.at[i, 0, pieces[c]],
                                  v_send.at[i, h, c], v_recv.at[i, 0, c], {"col": beside}))

    def via_arrival(i, leg, c):
        ref = via_ref.at[i, leg, pieces[c]]
        return pltpu.make_async_copy(ref, ref, v_recv.at[i, leg, c])

    def via_along():
        for i, way in enumerate((-1, 1)):
            on = detours(beside, r, 0, way) | detours(beside, r, 1, way)
            to = lax.rem(r + 2 * way + 2 * rows, rows)
            for c in range(CHUNKS):
                @pl.when(on)
                def _():
                    via_arrival(i, 0, c).wait()
                go(on, remote(via_ref.at[i, 0, pieces[c]], via_ref.at[i, 1, pieces[c]],
                              v_send.at[i, 2, c], v_recv.at[i, 1, c], {"row": to}))

    def via_back():
        for i, way in enumerate((-1, 1)):
            home = r - 2 * way
            second = detours(beside, home, 1, way)
            on = detours(beside, home, 0, way) | second
            k = lax.rem(2 * home + jnp.where(second, 1, 0) + 2 * panels, panels)
            for c in range(CHUNKS):
                @pl.when(on)
                def _():
                    via_arrival(i, 1, c).wait()
                go(on, remote(via_ref.at[i, 1, pieces[c]], ao_ref.at[k, pieces[c]],
                              v_send.at[i, 3, c], a_recv.at[k, c], {"col": beside}))
    for h in range(2):
        base = lax.rem(p - 2 * r - h + 2 * cols, cols)
        near = lax.rem(base - 1 + cols, cols)
        odd = lax.rem(base, 2)
        far = lax.rem(base - 2 * odd + cols, cols)
        go(near != p, remote(b_ref.at[h], bo_ref.at[h, 1], b_send.at[h, 0], b_recv.at[h, 1], {"col": near}))
        go(far != p, remote(b_ref.at[h], bo_ref.at[h, 2 * odd], b_send.at[h, 1], b_recv.at[h, 2 * odd], {"col": far}))

    def arrival(k, c):
        ref = ao_ref.at[k, pieces[c]]
        return pltpu.make_async_copy(ref, ref, a_recv.at[k, c])

    rest = []
    for d in range(1, rows):
        for h in range(2):
            above = lax.rem(2 * (r + d) + h, panels)
            below = lax.rem(2 * (r - d) + h + 2 * panels, panels)
            has_above = (r + d <= rows - 1) & carried(above, 0, r)
            has_below = (r - d >= 0) & carried(below, r, rows - 1)
            if d != 2:
                has_above = has_above & jnp.logical_not(detours(p, r + d, h, -1))
                has_below = has_below & jnp.logical_not(detours(p, r - d, h, 1))
            on_down = has_above & down_cond(above)
            on_up = has_below & up_cond(below)
            for c in range(CHUNKS):
                for on, k, hop_to in ((on_down, above, down_hop), (on_up, below, up_hop)):
                    if d < rows - 1:
                        @pl.when(on)
                        def _():
                            arrival(k, c).wait()
                        go(on, hop_to(ao_ref.at[k], k, h, d, c))
            for on, has, k in ((on_down, has_above, above), (on_up, has_below, below)):
                rest.append((has & jnp.logical_not(on) if d < rows - 1 else has, k))
        if d == 1:
            via_along()
    via_back()

    parity = lax.rem(p, 2)
    partner = p + 1 - 2 * parity

    def b_arrival(h, s):
        return pltpu.make_async_copy(bo_ref.at[h, s], bo_ref.at[h, s], b_recv.at[h, s])

    for h in range(2):
        home = lax.rem(p + 2 * r + h + 1, cols)

        @pl.when(home != p)
        def _():
            b_arrival(h, 1).wait()
        to_slot = 2 * parity
        for own_it in range(2):
            src = b_ref.at[h] if own_it else bo_ref.at[h, 1]
            here = (home == p) if own_it else ((home != p) & (home != partner))
            go(here, remote(src, bo_ref.at[h, to_slot], b_pass.at[h, own_it], b_recv.at[h, to_slot],
                            {"col": partner}))
    for h in range(2):
        for s in (0, 2):
            home = lax.rem(p + 2 * r + h + s, cols)

            @pl.when(home != p)
            def _():
                b_arrival(h, s).wait()
    for has, k in rest:
        @pl.when(has)
        def _():
            for c in range(CHUNKS):
                arrival(k, c).wait()
    for d in range(1, rows):
        pltpu.make_async_copy(ai_ref, aio_ref.at[0], ai_recv.at[d]).wait()
    for j in range(span):
        home = lax.rem(p + 2 * r + j, cols)

        @pl.when(home != p)
        def _():
            pltpu.make_async_copy(bi_ref, bio_ref.at[j], bi_recv.at[j]).wait()
    own_a.wait()
    for cond, copy in sends:
        @pl.when(cond)
        def _():
            copy.wait_send()


def multiply_kernel(rows, cols, steps, pairs_ref, count_ref, aid_ref, bid_ref, a_ref, ao_ref, b_ref, bo_ref, c_ref,
                    a_vm, b_vm, acc, out_vm, a_sem, b_sem, c_sem):
    p = lax.axis_index("col")
    r = lax.axis_index("row")
    panels = 2 * rows
    edge = acc.shape[-1]

    def load_a(j, act):
        k = lax.rem(p + 2 * r + j, panels)
        h = lax.rem(k, 2)

        @pl.when(k // 2 == r)
        def _():
            act(pltpu.make_async_copy(a_ref.at[h], a_vm.at[j], a_sem.at[j]))

        @pl.when(k // 2 != r)
        def _():
            act(pltpu.make_async_copy(ao_ref.at[k], a_vm.at[j], a_sem.at[j]))

    def load_b(h, s, act):
        k = lax.rem(p + 2 * r + h + s, cols)

        @pl.when(k == p)
        def _():
            act(pltpu.make_async_copy(b_ref.at[h], b_vm.at[h, s], b_sem.at[h, s]))

        @pl.when(k != p)
        def _():
            act(pltpu.make_async_copy(bo_ref.at[h, s], b_vm.at[h, s], b_sem.at[h, s]))

    start = lambda copy: copy.start()
    wait = lambda copy: copy.wait()
    for h in range(2):
        for s in range(steps):
            if h == 0 or s == steps - 1:
                load_a(h + s, start)
            load_b(h, s, start)
    outs = []
    for h in range(2):
        @pl.loop(0, WB * WB)
        def _(t):
            acc[t] = jnp.zeros(acc.shape[1:], acc.dtype)
        for s in range(steps):
            j = h + s
            if h == 0 or s == steps - 1:
                load_a(j, wait)
            load_b(h, s, wait)
            k = lax.rem(p + 2 * r + j, panels)

            def one(i):
                a = pairs_ref[h, s, 0, i]
                b = pairs_ref[h, s, 1, i]
                t = lax.rem(aid_ref[k, a], WB) * WB + lax.rem(bid_ref[2 * j + h, b], WB)
                return t, jnp.dot(a_vm[j, a], b_vm[h, s, b], preferred_element_type=jnp.float32)

            count = count_ref[h, s]

            @pl.loop(0, count // UNROLL)
            def _(i):
                found = [one(UNROLL * i + u) for u in range(UNROLL)]
                for t, value in found:
                    acc[t] += value

            @pl.loop(count // UNROLL * UNROLL, count)
            def _(i):
                t, value = one(i)
                acc[t] += value
        for row in range(WB):
            for col in range(WB):
                out_vm[h, row, :, col * edge:(col + 1) * edge] = acc[row * WB + col].astype(out_vm.dtype)
            copy = pltpu.make_async_copy(
                out_vm.at[h, row],
                c_ref.at[pl.ds(row * edge, edge), pl.ds(h * WB * edge, WB * edge)],
                c_sem.at[h, row])
            copy.start()
            outs.append(copy)
    for copy in outs:
        copy.wait()


def body(rows, cols, a_blocks, a_index, b_blocks, b_index, pair_list, pair_count):
    a, b = a_blocks[0], b_blocks[0]
    cap, edge = a.shape[1], a.shape[-1]
    steps = pair_list.shape[2]
    panel = (cap, edge, edge)
    dma = pltpu.SemaphoreType.DMA
    sds = jax.ShapeDtypeStruct
    ao, aio, bo, bio, _ = pl.pallas_call(
        functools.partial(move_kernel, rows, cols, steps),
        out_shape=(
            sds((2 * rows,) + panel, a.dtype),
            sds((rows, 2, cap), jnp.int32),
            sds((2, steps) + panel, b.dtype),
            sds((steps + 1, 2, cap), jnp.int32),
            sds((2, 2) + panel, a.dtype),
        ),
        in_specs=[ANY] * 4,
        out_specs=(ANY,) * 5,
        scratch_shapes=[
            dma((2 * rows, CHUNKS)), dma((rows, 2, CHUNKS)), dma((rows, 2, CHUNKS)), dma((rows,)), dma((rows,)),
            dma((2, steps)), dma((2, 2)), dma((2, 2)), dma((steps + 1,)), dma((steps + 1,)), dma((2,)),
            dma((2, 2, CHUNKS)), dma((2, 4, CHUNKS)),
        ],
        compiler_params=pltpu.CompilerParams(has_side_effects=True),
        name="move",
    )(a, a_index[0], b, b_index[0])
    return pl.pallas_call(
        functools.partial(multiply_kernel, rows, cols, steps),
        out_shape=sds((WB * edge, 2 * WB * edge), jnp.bfloat16),
        in_specs=[SMEM] * 4 + [ANY] * 4,
        out_specs=ANY,
        scratch_shapes=[
            pltpu.VMEM((steps + 1,) + panel, a.dtype),
            pltpu.VMEM((2, steps) + panel, b.dtype),
            pltpu.VMEM((WB * WB, edge, edge), jnp.float32),
            pltpu.VMEM((2, WB, edge, WB * edge), jnp.bfloat16),
            dma((steps + 1,)), dma((2, steps)), dma((2, WB)),
        ],
        compiler_params=pltpu.CompilerParams(vmem_limit_bytes=60000 * 1024),
        name="multiply",
    )(pair_list[0], pair_count[0], aio.reshape(2 * rows, cap), bio.reshape(2 * (steps + 1), cap), a, ao, b, bo)


def solution(mesh):
    in_specs = (
        P("col", "row", None, None, None),
        P("col", "row", None),
        P("col", "row", None, None, None),
        P("col", "row", None),
        P("col", "row", None, None, None),
        P("col", "row", None),
    )
    return jax.shard_map(
        functools.partial(body, mesh.shape["row"], mesh.shape["col"]),
        mesh=mesh, in_specs=in_specs, out_specs=P("col", "row"), check_vma=False)
```
